32 devices in a mesh: gx: 4 (over z), gy: 8 (over y, x, core).
Axes of the slice: x: 2, y: 2, z: 4, core: 2. Of those that a mesh axis runs over, the one named last changes fastest.
Arguments:
- gradient: float32 [32, 2048], P('gx', 'gy'), may hold values from -6 to 6
- warm_start: float32 [32, 2048], P('gx', 'gy'), may hold values from -3 to 3
- viscosity: float32 [32, 32, 2048], P(None, 'gx', 'gy'), may hold values from 1 to 10
- friction_coef: float32 [32, 2048], P('gx', 'gy'), may hold values from 0.5 to 5
- slide_dir: float32 [2, 32, 2048], P(None, 'gx', 'gy'), may hold values from -4 to 4
- obs_weight: float32 [32, 2048], P('gx', 'gy'), may hold values from 0.5 to 2
- ice_mask: int32 [32, 2048], P('gx', 'gy'), may hold values 0 or 1
- grounded: int32 [32, 2048], P('gx', 'gy'), may hold values 0 or 1
Outputs:
- solution: float32 [32, 2048], P('gx', 'gy')
- residual: float32 [32, 2048], P('gx', 'gy')
The draws below stay inside these ranges and needn't reach their ends.
All inputs are finite; a program needn't handle non-finite values. No bound on the sum of `ice_mask` or of `grounded` on one device may be relied on, other than what follows from the above.
Results may differ from the reference program's by a relative error of at most 0.00075.
Values sent between devices are 32-bit elements; how exact they have to be, the bound alone decides.
A program may use at most 128 MiB of HBM per device.

```python
import math
import jax
import jax.numpy as jnp

NZ = 32
ITERS = 2
NX = 32
NY = 2048


def plant(entries, rng, smallest, high):
    spot = [jax.random.randint(jax.random.fold_in(rng, axis), (), 0, length) for axis, length in enumerate(entries.shape)]
    longest = entries.shape.index(max(entries.shape))
    neighbour = spot[:longest] + [(spot[longest] + 1) % entries.shape[longest]] + spot[longest + 1:]
    return entries.at[tuple(spot)].set(smallest).at[tuple(neighbour)].set(high)


def block_levels(own_key, dims, shards, smallest, high):
    def one(dim, parts):
        steps = jax.random.uniform(jax.random.fold_in(jax.random.fold_in(own_key, 6), dim), (parts,), jnp.float32, smallest / len(shards), high / len(shards))
        return jnp.repeat(jnp.exp(steps), dims[dim] // parts).reshape((-1,) + (1,) * (len(dims) - dim - 1))

    gain = one(*shards[0])
    for cut in shards[1:]:
        gain = gain * one(*cut)
    return gain


def normal_values(key, dims, scale, limit, pieces=(), kind=jnp.bfloat16):
    values = jax.random.normal(key, dims, jnp.float32) * scale
    if len(pieces) > 0:
        values = block_levels(key, dims, pieces, -0.22, 0.18) * values
    return jnp.clip(values, min=-limit, max=limit).astype(kind)


def setup_inputs(seed: int = 0) -> dict:
    keys = jax.random.split(jax.random.key(seed), 9)
    gradient = normal_values(keys[0], (NX, NY), 1.0, 6.0, ((0, 4), (1, 8)), jnp.float32)
    warm_start = normal_values(keys[1], (NX, NY), 0.5, 3.0, ((0, 4), (1, 8)), jnp.float32)
    viscosity = jnp.clip(jnp.exp(math.log(10.0) - 2.3025851 * jax.random.uniform(keys[2], (NZ, NX, NY), jnp.float32) ** block_levels(keys[2], (NZ, NX, NY), ((1, 4), (2, 8)), -0.2, 0.2)), 1.0, 10.0)
    friction_coef = jnp.clip(jnp.exp(math.log(5.0) - 2.3025851 * jax.random.uniform(keys[3], (NX, NY), jnp.float32) ** block_levels(keys[3], (NX, NY), ((0, 4), (1, 8)), -0.2, 0.2)), 0.5, 5.0)
    slide_dir = normal_values(keys[4], (2, NX, NY), 1.0, 4.0, ((1, 4), (2, 8)), jnp.float32)
    obs_weight = jnp.clip(jnp.exp(math.log(2.0) - 1.3862944 * jax.random.uniform(keys[5], (NX, NY), jnp.float32) ** block_levels(keys[5], (NX, NY), ((0, 4), (1, 8)), -0.2, 0.2)), 0.5, 2.0)
    ice_mask = plant((jax.random.randint(keys[6], (NX, NY), 0, 8) < 7).astype(jnp.int32), jax.random.fold_in(keys[6], 1), 0, 1)
    grounded = plant((jax.random.randint(keys[7], (NX, NY), 0, 4) < 3).astype(jnp.int32), jax.random.fold_in(keys[7], 1), 0, 1)
    return {"gradient": gradient, "warm_start": warm_start, "viscosity": viscosity, "friction_coef": friction_coef, "slide_dir": slide_dir, "obs_weight": obs_weight, "ice_mask": ice_mask, "grounded": grounded}


vert_coupling = 128.0
sink_rate = 0.0625
bed_drag = 0.5
offset_weight = 0.0019
cross_share = 0.5
reg_gamma = 0.02
reg_smooth = 1.0
diag_scale = 0.003

neighbour_offsets = [(step_z, step_x, step_y) for step_z in (-1, 0, 1) for step_x in (-1, 0, 1) for step_y in (-1, 0, 1) if step_x != 0 or step_y != 0]


def couple(field_ext, eta_ext):
    levels = eta_ext.shape[0]
    span_x = eta_ext.shape[1] - 2
    span_y = eta_ext.shape[2] - 2
    padded_field = jnp.pad(field_ext, ((0, 0), (1, 1), (0, 0), (0, 0)))
    padded_eta = jnp.pad(eta_ext, ((1, 1), (0, 0), (0, 0)))
    center = eta_ext[:, 1:1 + span_x, 1:1 + span_y]
    along_one = jnp.zeros((levels, span_x, span_y), jnp.float32)
    along_two = jnp.zeros((levels, span_x, span_y), jnp.float32)
    for step_z, step_x, step_y in neighbour_offsets:
        near_eta = padded_eta[1 + step_z:1 + step_z + levels, 1 + step_x:1 + step_x + span_x, 1 + step_y:1 + step_y + span_y]
        weight = (offset_weight / (abs(step_x) + abs(step_y) + abs(step_z))) * 0.5 * (center + near_eta)
        near_field = padded_field[:, 1 + step_z:1 + step_z + levels, 1 + step_x:1 + step_x + span_x, 1 + step_y:1 + step_y + span_y]
        along_one = along_one + weight * near_field[0]
        along_two = along_two + weight * near_field[1]
        if step_x != 0 and step_y != 0:
            twist_weight = (cross_share * step_x * step_y) * weight
            along_one = along_one + twist_weight * near_field[1]
            along_two = along_two + twist_weight * near_field[0]
    return jnp.stack([along_one, along_two])


def tridiagonal(link_weights, diagonal, rhs_cols):
    levels = diagonal.shape[0]
    pivot_value = diagonal[0]
    ratios = [-link_weights[0] / pivot_value]
    partial_value = [rhs_cols[:, 0] / pivot_value]
    for layer_index in range(1, levels):
        pivot_value = diagonal[layer_index] + link_weights[layer_index - 1] * ratios[-1]
        partial_value.append((rhs_cols[:, layer_index] + link_weights[layer_index - 1] * partial_value[-1]) / pivot_value)
        if layer_index < levels - 1:
            ratios.append(-link_weights[layer_index] / pivot_value)
    result = [partial_value[-1]]
    for layer_index in range(levels - 2, -1, -1):
        result.insert(0, partial_value[layer_index] - ratios[layer_index] * result[0])
    return jnp.stack(result, axis=1)


def responses(viscosity, friction):
    levels = viscosity.shape[0]
    link_weights = vert_coupling * 0.5 * (viscosity[:-1] + viscosity[1:])
    zero_layer = jnp.zeros_like(viscosity[:1])
    diagonal = jnp.concatenate([zero_layer, link_weights]) + jnp.concatenate([link_weights, zero_layer]) + sink_rate * viscosity
    diagonal = diagonal.at[0].add(bed_drag * friction)
    unit_rhs = jnp.zeros((2,) + viscosity.shape, jnp.float32)
    unit_rhs = unit_rhs.at[0, 0].set(1.0).at[1, levels - 1].set(1.0)
    solved = tridiagonal(link_weights, diagonal, unit_rhs)
    return solved[0], solved[1]


def regularize(centre_ext):
    middle = centre_ext[1:-1, 1:-1]
    beside_all = centre_ext[2:, 1:-1] + centre_ext[:-2, 1:-1] + centre_ext[1:-1, 2:] + centre_ext[1:-1, :-2]
    return reg_gamma * (middle + reg_smooth * (4.0 * middle - beside_all))


def reference(gradient, warm_start, viscosity, friction_coef, slide_dir, obs_weight, ice_mask, grounded):
    ice_float = ice_mask.astype(jnp.float32)
    ground_float = grounded.astype(jnp.float32)
    friction = ground_float * friction_coef
    source = (ice_float * ground_float * friction_coef)[None] * slide_dir
    obs = ice_float * obs_weight
    inverse_diag = 1.0 / (reg_gamma * (1.0 + 4.0 * reg_smooth) + diag_scale * ice_float * ground_float * friction_coef * friction_coef)
    bottom_resp, top_resp = responses(viscosity, friction)
    eta_ext = jnp.pad(viscosity, ((0, 0), (1, 1), (1, 1)))

    def hessian(direction):
        spread = source * direction[None]
        first_state = bottom_resp[None] * spread[:, None]
        coupled = couple(jnp.pad(first_state, ((0, 0), (0, 0), (1, 1), (1, 1))), eta_ext)
        surface = spread * bottom_resp[-1][None] + jnp.sum(top_resp[None] * coupled, axis=1)
        traction = obs[None] * surface
        second_state = top_resp[None] * traction[:, None]
        coupled_back = couple(jnp.pad(second_state, ((0, 0), (0, 0), (1, 1), (1, 1))), eta_ext)
        basal_part = traction * top_resp[0][None] + jnp.sum(bottom_resp[None] * coupled_back, axis=1)
        return jnp.sum(source * basal_part, axis=0) + regularize(jnp.pad(direction, 1))

    solution = warm_start
    residual = gradient - hessian(warm_start)
    precond = inverse_diag * residual
    direction = precond
    norm_now = jnp.sum(residual * precond)
    for iteration in range(ITERS):
        image_vec = hessian(direction)
        step_size = norm_now / jnp.sum(direction * image_vec)
        solution = solution + step_size * direction
        residual = residual - step_size * image_vec
        precond = inverse_diag * residual
        norm_next = jnp.sum(residual * precond)
        direction = precond + (norm_next / norm_now) * direction
        norm_now = norm_next
    return solution, residual
```

```python
import functools

import jax
import jax.numpy as jnp
from jax import lax
from jax.experimental import pallas as pl
from jax.experimental.pallas import tpu as pltpu
from jax.sharding import PartitionSpec as P

vert_coupling = 128.0
sink_rate = 0.0625
bed_drag = 0.5
offset_weight = 0.0019
cross_share = 0.5
reg_gamma = 0.02
reg_smooth = 1.0
diag_scale = 0.003

MESH = pl.DeviceIdType.MESH
REACH = 6
DIRS = [(-1, 0), (1, 0), (0, -1), (0, 1), (-1, -1), (-1, 1), (1, -1), (1, 1)]
OPPOSITE = [1, 0, 3, 2, 7, 6, 5, 4]
FIELDS = 7


def roll(x, shift, axis):
    size = x.shape[axis]
    if isinstance(shift, int):
        shift = shift % size
        if shift == 0:
            return x
    return pltpu.roll(x, shift, axis)


def near(x, step, axis):
    return roll(x, -step, axis)


def kernel(
    nx, ny,
    grad_ref, warm_ref, visc_ref, fric_ref, slide_ref, obs_ref, ice_ref, ground_ref,
    sol_ref, res_ref,
    up, down, bot, gbot, top, gtop,
    row_send, row_recv, f_send, f_recv, p_send, p_recv, k_send, k_recv, kp_send, kp_recv,
    ext, red, slots,
    s_send, s_recv, r_send, r_recv,
):
    levels, rows, cols = visc_ref.shape
    n = nx * ny
    ix, iy = lax.axis_index("gx"), lax.axis_index("gy")
    me = ix * ny + iy

    barrier = pltpu.get_barrier_semaphore()

    def greet(j, c):
        peer = lax.rem(me + j, n)
        pl.semaphore_signal(barrier, inc=1, device_id=(peer // ny, lax.rem(peer, ny)), device_id_type=MESH)
        return c

    lax.fori_loop(1, n, greet, 0)

    def exists(d):
        dx, dy = DIRS[d]
        x, y = ix + dx, iy + dy
        return (x >= 0) & (x < nx) & (y >= 0) & (y < ny)

    def copy(src, dst, d, sem):
        dx, dy = DIRS[d]
        return pltpu.make_async_remote_copy(
            src_ref=src, dst_ref=dst,
            send_sem=s_send.at[sem + d], recv_sem=s_recv.at[sem + OPPOSITE[d]],
            device_id=(jnp.clip(ix + dx, 0, nx - 1), jnp.clip(iy + dy, 0, ny - 1)),
            device_id_type=MESH,
        )

    def messages(d, stage):
        o = OPPOSITE[d]
        side = 0 if DIRS[d][1] < 0 else 1
        if stage == 0:
            if d < 2:
                return [copy(row_send.at[d], row_recv.at[o], d, 0), copy(f_send, f_recv.at[o], d, 8)]
            return [copy(p_send.at[side], p_recv.at[o - 2], d, 0)]
        if d < 2:
            return [copy(k_send, k_recv.at[o], d, 16)]
        return [copy(kp_send.at[side], kp_recv.at[o - 2], d, 16)]

    def clear(d, stage):
        if stage == 0:
            refs = [row_recv.at[d], f_recv.at[d]] if d < 2 else [p_recv.at[d - 2]]
        else:
            refs = [k_recv.at[d]] if d < 2 else [kp_recv.at[d - 2]]
        for ref in refs:
            ref[...] = jnp.zeros(ref.shape, jnp.float32)

    def start(stage):
        for d in range(8):
            @pl.when(exists(d))
            def _():
                for m in messages(d, stage):
                    m.start()

    def finish_recv(stage):
        for d in range(8):
            @pl.when(exists(d))
            def _():
                o = OPPOSITE[d]
                for m in messages(o, stage):
                    m.wait_recv()

    def finish_send(stage):
        for d in range(8):
            @pl.when(exists(d))
            def _():
                for m in messages(d, stage):
                    m.wait_send()

    for stage in (0, 1):
        for d in range(8):
            @pl.when(jnp.logical_not(exists(d)))
            def _():
                clear(d, stage)

    ice = ice_ref[...].astype(jnp.float32)
    ground = ground_ref[...].astype(jnp.float32)
    fric = fric_ref[...]
    friction = ground * fric
    base = ice * ground * fric
    inverse = 1.0 / (reg_gamma * (1.0 + 4.0 * reg_smooth) + diag_scale * base * fric)
    lane = lax.broadcasted_iota(jnp.int32, (rows, 128), 1)

    def eliminate(i, carry):
        e, f = carry
        k = levels - 2 - i
        v_low, v_up = visc_ref[i], visc_ref[i + 1]
        link = (vert_coupling * 0.5) * (v_low + v_up)
        ratio = link / (link + e)
        up[i] = ratio
        e = sink_rate * v_up + e * ratio
        w_low, w_up = visc_ref[k], visc_ref[k + 1]
        link = (vert_coupling * 0.5) * (w_low + w_up)
        ratio = link / (link + f)
        down[k] = ratio
        f = sink_rate * w_low + f * ratio
        return e, f

    e = sink_rate * visc_ref[0] + bed_drag * friction
    f = sink_rate * visc_ref[levels - 1]
    e, f = lax.fori_loop(0, levels - 1, eliminate, (e, f))

    zero = jnp.zeros((rows, cols), jnp.float32)
    for ref in (top, gtop):
        ref[0] = zero
        ref[levels + 1] = zero

    def respond(z, carry):
        b, t, left, right = carry
        g = visc_ref[z] * b
        bot[z] = b
        gbot[z] = g
        for j, val in ((0, b), (levels, g)):
            row_send[0, pl.ds(z + j, 1), :] = val[:1]
            row_send[1, pl.ds(z + j, 1), :] = val[rows - 1:]
            left = jnp.where(lane == z + j, roll(val[:, :128], z + j, 1), left)
            right = jnp.where(lane == z + j, roll(val[:, cols - 128:], z + j + 1, 1), right)
        k = levels - 1 - z
        top[k + 1] = t
        gtop[k + 1] = visc_ref[k] * t
        t = t * up[jnp.maximum(k - 1, 0)]
        b = b * down[jnp.minimum(z, levels - 2)]
        return b, t, left, right

    blank = jnp.zeros((rows, 128), jnp.float32)
    _, _, left, right = lax.fori_loop(
        0, levels, respond, (1.0 / (f + bed_drag * friction), 1.0 / e, blank, blank)
    )

    own = [base * slide_ref[0], base * slide_ref[1], ice * obs_ref[...], inverse, bot[levels - 1], warm_ref[...], grad_ref[...]]

    def pack(fields, place, left, right):
        for val in fields:
            here = (lane >= place) & (lane < place + REACH)
            left = jnp.where(here, roll(val[:, :128], place, 1), left)
            right = jnp.where(here, roll(val[:, cols - 128:], place - (128 - REACH), 1), right)
            place += REACH
        return left, right

    left, right = pack(own, 2 * levels, left, right)
    for j, val in enumerate(own):
        f_send[j] = val
    p_send[0] = left
    p_send[1] = right

    pl.semaphore_wait(barrier, n - 1)
    start(0)
    finish_recv(0)

    row_id = lax.broadcasted_iota(jnp.int32, (rows, cols), 0)
    col_id = lax.broadcasted_iota(jnp.int32, (rows, cols), 1)
    prow = lax.broadcasted_iota(jnp.int32, (rows, 128), 0)

    def beside(side):
        at = {dx: p_recv[DIRS.index((dx, side)) - 2] for dx in (-1, 0, 1)}
        return {
            -1: jnp.where(prow == 0, near(at[-1], -1, 0), near(at[0], -1, 0)),
            0: at[0],
            1: jnp.where(prow == rows - 1, near(at[1], 1, 0), near(at[0], 1, 0)),
        }

    packs = {side: beside(side) for side in (-1, 1)}

    def gather(z, acc):
        acc = list(acc)
        weights = []
        for ref in (gtop, top):
            mid, out = ref[z + 1], ref[z] + ref[z + 2]
            weights.append((
                (0.5 * offset_weight) * mid + (0.25 * offset_weight) * out,
                (0.25 * offset_weight) * mid + (0.5 * offset_weight / 3.0) * out,
            ))
        for j, ref, weight in ((0, bot, weights[0]), (levels, gbot, weights[1])):
            mid = ref[z]
            low = jnp.where(row_id == 0, row_recv[0, pl.ds(z + j, 1), :], near(mid, -1, 0))
            high = jnp.where(row_id == rows - 1, row_recv[1, pl.ds(z + j, 1), :], near(mid, 1, 0))
            for dx, val in ((-1, low), (0, mid), (1, high)):
                from_left = roll(packs[-1][dx], lax.rem(128 - z - j, 128), 1)
                from_right = roll(packs[1][dx], 127 - z - j, 1)
                wide = lambda x: jnp.concatenate([x] * (cols // 128), axis=1)
                sides = {
                    -1: jnp.where(col_id == 0, wide(from_left), near(val, -1, 1)),
                    0: val,
                    1: jnp.where(col_id == cols - 1, wide(from_right), near(val, 1, 1)),
                }
                for dy in (-1, 0, 1):
                    if (dx, dy) != (0, 0):
                        d = DIRS.index((dx, dy))
                        acc[d] = acc[d] + weight[1 if dx * dy != 0 else 0] * sides[dy]
        return tuple(acc)

    coefs = lax.fori_loop(0, levels, gather, (zero,) * 8)
    for d in range(8):
        k_send[d] = coefs[d]
    kleft, kright = pack(coefs, 0, blank, blank)
    kp_send[0] = kleft
    kp_send[1] = kright
    start(1)

    def extend(j, mine, recv, packs_ref, index, place):
        for tile, dx in enumerate((-1, 0, 1)):
            here = mine if dx == 0 else recv[0 if dx < 0 else 1, index]
            from_right = packs_ref[DIRS.index((dx, 1)) - 2]
            from_left = packs_ref[DIRS.index((dx, -1)) - 2]
            halo = jnp.where(lane < REACH, roll(from_right, -place, 1), 0.0)
            halo = jnp.where(lane >= 128 - REACH, roll(from_left, 128 - REACH - place, 1), halo)
            ext[j, tile * rows:(tile + 1) * rows, :cols] = here
            ext[j, tile * rows:(tile + 1) * rows, cols:] = halo

    for j in range(FIELDS):
        extend(j, f_send[j], f_recv, p_recv, j, 2 * levels + REACH * j)
    finish_recv(1)
    for d in range(8):
        extend(FIELDS + d, k_send[d], k_recv, kp_recv, d, REACH * d)

    def coef(dx, dy):
        return ext[FIELDS + DIRS.index((dx, dy))]

    def hessian(q):
        spread = [ext[0] * q, ext[1] * q]
        surface = [ext[4] * spread[0], ext[4] * spread[1]]
        for dx in (-1, 0, 1):
            moved = [near(s, dx, 0) for s in spread]
            for dy in (-1, 0, 1):
                if (dx, dy) == (0, 0):
                    continue
                share = cross_share * dx * dy
                for c in range(2):
                    val = moved[c] if share == 0 else moved[c] + share * moved[1 - c]
                    surface[c] = surface[c] + coef(dx, dy) * near(val, dy, 1)
        traction = [ext[2] * s for s in surface]
        basal = [ext[4] * t for t in traction]
        for dx in (-1, 0, 1):
            part = [None, None]
            for dy in (-1, 0, 1):
                if (dx, dy) == (0, 0):
                    continue
                share = cross_share * dx * dy
                for c in range(2):
                    val = traction[c] if share == 0 else traction[c] + share * traction[1 - c]
                    val = near(coef(-dx, -dy) * val, dy, 1)
                    part[c] = val if part[c] is None else part[c] + val
            basal = [basal[c] + near(part[c], dx, 0) for c in range(2)]
        around = near(q, 1, 0) + near(q, -1, 0) + near(q, 1, 1) + near(q, -1, 1)
        smooth = reg_gamma * (q + reg_smooth * (4.0 * q - around))
        return ext[0] * basal[0] + ext[1] * basal[1] + smooth

    def mine(x):
        return x[rows:2 * rows, :cols]

    warm = ext[5]
    r0 = ext[6] - hessian(warm)
    p0 = ext[3] * r0
    w0 = hessian(p0)
    y0 = ext[3] * w0
    u0 = mine(hessian(y0))
    r0, p0, w0, y0 = mine(r0), mine(p0), mine(w0), mine(y0)

    def total(x):
        return jnp.sum(jnp.sum(x, axis=0, keepdims=True), axis=1, keepdims=True)

    one_lane = lax.broadcasted_iota(jnp.int32, (1, 128), 1)
    sums = jnp.zeros((1, 128), jnp.float32)
    for j, val in enumerate((r0 * p0, p0 * w0, w0 * y0, y0 * u0)):
        sums = jnp.where(one_lane == j, total(val), sums)
    red[...] = sums

    def to_peer(j, index):
        peer = lax.rem(me + j, n)
        return pltpu.make_async_remote_copy(
            src_ref=red, dst_ref=slots.at[index],
            send_sem=r_send.at[j], recv_sem=r_recv.at[index],
            device_id=(peer // ny, lax.rem(peer, ny)), device_id_type=MESH,
        )

    def send(j, c):
        to_peer(j, me).start()
        return c

    def receive(j, c):
        to_peer(j, lax.rem(me + j, n)).wait_recv()
        return c

    def sent(j, c):
        to_peer(j, me).wait_send()
        return c

    lax.fori_loop(1, n, send, 0)
    lax.fori_loop(1, n, receive, 0)
    slots[me] = sums
    everyone = jnp.sum(slots[...], axis=0)

    def pick(j):
        return jnp.sum(jnp.where(one_lane == j, everyone, 0.0), axis=1, keepdims=True)

    rz0, pw, wy, yu = pick(0), pick(1), pick(2), pick(3)
    a0 = rz0 / pw
    rz1 = a0 * a0 * wy - rz0
    beta = rz1 / rz0
    more = 1.0 + beta
    curve = more * (more * pw - 2.0 * a0 * wy) + a0 * a0 * yu
    a1 = rz1 / curve
    sol_ref[...] = warm_ref[...] + a0 * p0 + a1 * (more * p0 - a0 * y0)
    res_ref[...] = r0 - a0 * w0 - a1 * (more * w0 - a0 * u0)

    finish_send(0)
    finish_send(1)
    lax.fori_loop(1, n, sent, 0)


def solution(mesh):
    nx, ny = mesh.shape["gx"], mesh.shape["gy"]
    n = nx * ny

    def on_device(gradient, warm_start, viscosity, friction_coef, slide_dir, obs_weight, ice_mask, grounded):
        levels, rows, cols = viscosity.shape
        vmem = pl.BlockSpec(memory_space=pltpu.VMEM)
        f32 = lambda *shape: pltpu.VMEM(shape, jnp.float32)
        return tuple(pl.pallas_call(
            functools.partial(kernel, nx, ny),
            out_shape=[jax.ShapeDtypeStruct((rows, cols), jnp.float32)] * 2,
            in_specs=[vmem] * 8,
            out_specs=[vmem] * 2,
            scratch_shapes=[
                f32(levels, rows, cols), f32(levels, rows, cols),
                f32(levels, rows, cols), f32(levels, rows, cols),
                f32(levels + 2, rows, cols), f32(levels + 2, rows, cols),
                f32(2, 2 * levels, cols), f32(2, 2 * levels, cols),
                f32(FIELDS, rows, cols), f32(2, FIELDS, rows, cols),
                f32(2, rows, 128), f32(6, rows, 128),
                f32(8, rows, cols), f32(2, 8, rows, cols),
                f32(2, rows, 128), f32(6, rows, 128),
                f32(FIELDS + 8, 3 * rows, cols + 128),
                f32(1, 128), f32(n, 1, 128),
                pltpu.SemaphoreType.DMA((24,)), pltpu.SemaphoreType.DMA((24,)),
                pltpu.SemaphoreType.DMA((n,)), pltpu.SemaphoreType.DMA((n,)),
            ],
            compiler_params=pltpu.CompilerParams(collective_id=0, has_side_effects=True),
        )(gradient, warm_start, viscosity, friction_coef, slide_dir, obs_weight, ice_mask, grounded))

    flat = P("gx", "gy")
    deep = P(None, "gx", "gy")
    return jax.shard_map(
        on_device,
        mesh=mesh,
        in_specs=(flat, flat, deep, flat, deep, flat, flat, flat),
        out_specs=(flat, flat),
        check_vma=False,
    )
```

```python
import functools

import jax
import jax.numpy as jnp
from jax import lax
from jax.experimental import pallas as pl
from jax.experimental.pallas import tpu as pltpu
from jax.sharding import PartitionSpec as P

vert_coupling = 128.0
sink_rate = 0.0625
bed_drag = 0.5
offset_weight = 0.0019
cross_share = 0.5
reg_gamma = 0.02
reg_smooth = 1.0
diag_scale = 0.003

MESH = pl.DeviceIdType.MESH
REACH = 6
DIRS = [(-1, 0), (1, 0), (0, -1), (0, 1), (-1, -1), (-1, 1), (1, -1), (1, 1)]
OPPOSITE = [1, 0, 3, 2, 7, 6, 5, 4]
FIELDS = 7


def roll(x, shift, axis):
    size = x.shape[axis]
    if isinstance(shift, int):
        shift = shift % size
        if shift == 0:
            return x
    return pltpu.roll(x, shift, axis)


def near(x, step, axis):
    return roll(x, -step, axis)


def kernel(
    nx, ny,
    grad_in, warm_in, visc_in, fric_in, slide_in, obs_in, ice_in, ground_in,
    out_ref,
    grad_ref, warm_ref, visc_ref, fric_ref, slide_ref, obs_ref, ice_ref, ground_ref,
    up, down, bot, gbot, top, gtop,
    row_send, row_recv, f_send, f_recv, p_send, p_recv, k_send, k_recv, kp_send, kp_recv,
    ext, red, slots,
    load_sem, s_send, s_recv, r_send, r_recv, all_in,
):
    levels, rows, cols = visc_ref.shape
    n = nx * ny
    ix, iy = lax.axis_index("gx"), lax.axis_index("gy")
    me = ix * ny + iy

    loads = [
        pltpu.make_async_copy(src, dst, load_sem.at[j])
        for j, (src, dst) in enumerate((
            (visc_in, visc_ref), (fric_in, fric_ref), (ground_in, ground_ref), (ice_in, ice_ref),
            (slide_in, slide_ref), (obs_in, obs_ref), (warm_in, warm_ref), (grad_in, grad_ref),
        ))
    ]

    def exists(d):
        dx, dy = DIRS[d]
        x, y = ix + dx, iy + dy
        return (x >= 0) & (x < nx) & (y >= 0) & (y < ny)

    barrier = pltpu.get_barrier_semaphore()

    def greet(x, y):
        pl.semaphore_signal(barrier, inc=1, device_id=(x, y), device_id_type=MESH)

    for load in loads:
        load.start()
    expected = nx - 1 + ny - 1
    for d in range(4, 8):
        expected = expected + exists(d).astype(jnp.int32)

        @pl.when(exists(d))
        def _():
            greet(ix + DIRS[d][0], iy + DIRS[d][1])
    for k in range(1, nx):
        greet(lax.rem(ix + k, nx), iy)
    for k in range(1, ny):
        greet(ix, lax.rem(iy + k, ny))

    def copy(src, dst, d, sem):
        dx, dy = DIRS[d]
        return pltpu.make_async_remote_copy(
            src_ref=src, dst_ref=dst,
            send_sem=s_send.at[sem + d], recv_sem=s_recv.at[sem + OPPOSITE[d]],
            device_id=(jnp.clip(ix + dx, 0, nx - 1), jnp.clip(iy + dy, 0, ny - 1)),
            device_id_type=MESH,
        )

    def message(d, what):
        o = OPPOSITE[d]
        side = 0 if DIRS[d][1] < 0 else 1
        return {
            "row": lambda: copy(row_send.at[d], row_recv.at[o], d, 0),
            "field": lambda: copy(f_send, f_recv.at[o], d, 8),
            "coef": lambda: copy(k_send, k_recv.at[o], d, 16),
            "pack": lambda: copy(p_send.at[side], p_recv.at[o - 2], d, 0),
            "coefpack": lambda: copy(kp_send.at[side], kp_recv.at[o - 2], d, 16),
        }[what]()

    beside_x, others = (0, 1), range(2, 8)
    kinds = (("row", beside_x), ("pack", others), ("field", beside_x), ("coefpack", others), ("coef", beside_x))

    def each(action, names):
        for name, towards in kinds:
            if name not in names:
                continue
            for d in towards:
                @pl.when(exists(d))
                def _():
                    if action == "wait_recv":
                        message(OPPOSITE[d], name).wait_recv()
                    elif action == "wait_send":
                        message(d, name).wait_send()
                    else:
                        message(d, name).start()

    def clear(ref):
        ref[...] = jnp.zeros(ref.shape, jnp.float32)

    for d in range(8):
        @pl.when(jnp.logical_not(exists(d)))
        def _():
            for ref in (row_recv, f_recv, k_recv) if d < 2 else (p_recv, kp_recv):
                clear(ref.at[d if d < 2 else d - 2])

    for load in loads:
        load.wait()

    ice = ice_ref[...].astype(jnp.float32)
    ground = ground_ref[...].astype(jnp.float32)
    fric = fric_ref[...]
    friction = ground * fric
    base = ice * ground * fric
    inverse = 1.0 / (reg_gamma * (1.0 + 4.0 * reg_smooth) + diag_scale * base * fric)
    lane = lax.broadcasted_iota(jnp.int32, (rows, 128), 1)

    def eliminate(i, carry):
        e, f = carry
        k = levels - 2 - i
        v_low, v_up = visc_ref[i], visc_ref[i + 1]
        link = (vert_coupling * 0.5) * (v_low + v_up)
        ratio = link / (link + e)
        up[i] = ratio
        e = sink_rate * v_up + e * ratio
        w_low, w_up = visc_ref[k], visc_ref[k + 1]
        link = (vert_coupling * 0.5) * (w_low + w_up)
        ratio = link / (link + f)
        down[k] = ratio
        f = sink_rate * w_low + f * ratio
        return e, f

    e = sink_rate * visc_ref[0] + bed_drag * friction
    f = sink_rate * visc_ref[levels - 1]
    e, f = lax.fori_loop(0, levels - 1, eliminate, (e, f), unroll=True)

    zero = jnp.zeros((rows, cols), jnp.float32)
    for ref in (top, gtop):
        ref[0] = zero
        ref[levels + 1] = zero

    def respond(z, carry):
        b, t, left, right = carry
        g = visc_ref[z] * b
        bot[z] = b
        gbot[z] = g
        for j, val in ((0, b), (levels, g)):
            row_send[0, pl.ds(z + j, 1), :] = val[:1]
            row_send[1, pl.ds(z + j, 1), :] = val[rows - 1:]
            left = jnp.where(lane == z + j, roll(val[:, :128], z + j, 1), left)
            right = jnp.where(lane == z + j, roll(val[:, cols - 128:], z + j + 1, 1), right)
        k = levels - 1 - z
        top[k + 1] = t
        gtop[k + 1] = visc_ref[k] * t
        t = t * up[jnp.maximum(k - 1, 0)]
        b = b * down[jnp.minimum(z, levels - 2)]
        return b, t, left, right

    blank = jnp.zeros((rows, 128), jnp.float32)
    _, _, left, right = lax.fori_loop(
        0, levels, respond, (1.0 / (f + bed_drag * friction), 1.0 / e, blank, blank), unroll=4
    )

    own = [base * slide_ref[0], base * slide_ref[1], ice * obs_ref[...], inverse, bot[levels - 1], warm_ref[...], grad_ref[...]]

    def pack(fields, place, left, right):
        for val in fields:
            here = (lane >= place) & (lane < place + REACH)
            left = jnp.where(here, roll(val[:, :128], place, 1), left)
            right = jnp.where(here, roll(val[:, cols - 128:], place - (128 - REACH), 1), right)
            place += REACH
        return left, right

    left, right = pack(own, 2 * levels, left, right)
    for j, val in enumerate(own):
        f_send[j] = val
    p_send[0] = left
    p_send[1] = right

    pl.semaphore_wait(barrier, expected)
    each("start", ("row", "pack", "field"))
    for k in range(1, ny):
        pl.semaphore_signal(all_in, inc=1, device_id=(ix, lax.rem(iy + k, ny)), device_id_type=MESH)
    each("wait_recv", ("row", "pack"))

    row_id = lax.broadcasted_iota(jnp.int32, (rows, cols), 0)
    col_id = lax.broadcasted_iota(jnp.int32, (rows, cols), 1)
    prow = lax.broadcasted_iota(jnp.int32, (rows, 128), 0)

    def beside(side):
        at = {dx: p_recv[DIRS.index((dx, side)) - 2] for dx in (-1, 0, 1)}
        return {
            -1: jnp.where(prow == 0, near(at[-1], -1, 0), near(at[0], -1, 0)),
            0: at[0],
            1: jnp.where(prow == rows - 1, near(at[1], 1, 0), near(at[0], 1, 0)),
        }

    packs = {side: beside(side) for side in (-1, 1)}

    def gather(z, acc):
        acc = list(acc)
        weights = []
        for ref in (gtop, top):
            mid, out = ref[z + 1], ref[z] + ref[z + 2]
            weights.append((
                (0.5 * offset_weight) * mid + (0.25 * offset_weight) * out,
                (0.25 * offset_weight) * mid + (0.5 * offset_weight / 3.0) * out,
            ))
        for j, ref, weight in ((0, bot, weights[0]), (levels, gbot, weights[1])):
            mid = ref[z]
            low = jnp.where(row_id == 0, row_recv[0, pl.ds(z + j, 1), :], near(mid, -1, 0))
            high = jnp.where(row_id == rows - 1, row_recv[1, pl.ds(z + j, 1), :], near(mid, 1, 0))
            for dx, val in ((-1, low), (0, mid), (1, high)):
                from_left = roll(packs[-1][dx], lax.rem(128 - z - j, 128), 1)
                from_right = roll(packs[1][dx], 127 - z - j, 1)
                wide = lambda x: jnp.concatenate([x] * (cols // 128), axis=1)
                sides = {
                    -1: jnp.where(col_id == 0, wide(from_left), near(val, -1, 1)),
                    0: val,
                    1: jnp.where(col_id == cols - 1, wide(from_right), near(val, 1, 1)),
                }
                for dy in (-1, 0, 1):
                    if (dx, dy) != (0, 0):
                        d = DIRS.index((dx, dy))
                        acc[d] = acc[d] + weight[1 if dx * dy != 0 else 0] * sides[dy]
        return tuple(acc)

    coefs = lax.fori_loop(0, levels, gather, (zero,) * 8, unroll=4)
    for d in range(8):
        k_send[d] = coefs[d]
    kleft, kright = pack(coefs, 0, blank, blank)
    kp_send[0] = kleft
    kp_send[1] = kright
    each("start", ("coefpack", "coef"))

    def extend(j, mine, recv, packs_ref, index, place):
        for tile, dx in enumerate((-1, 0, 1)):
            here = mine if dx == 0 else recv[0 if dx < 0 else 1, index]
            from_right = packs_ref[DIRS.index((dx, 1)) - 2]
            from_left = packs_ref[DIRS.index((dx, -1)) - 2]
            halo = jnp.where(lane < REACH, roll(from_right, -place, 1), 0.0)
            halo = jnp.where(lane >= 128 - REACH, roll(from_left, 128 - REACH - place, 1), halo)
            ext[j, tile * rows:(tile + 1) * rows, :cols] = here
            ext[j, tile * rows:(tile + 1) * rows, cols:] = halo

    each("wait_recv", ("field",))
    for j in range(FIELDS):
        extend(j, f_send[j], f_recv, p_recv, j, 2 * levels + REACH * j)
    each("wait_recv", ("coefpack", "coef"))
    for d in range(8):
        extend(FIELDS + d, k_send[d], k_recv, kp_recv, d, REACH * d)

    def coef(dx, dy):
        return ext[FIELDS + DIRS.index((dx, dy))]

    def forth(q):
        spread = [ext[0] * q, ext[1] * q]
        surface = [ext[4] * spread[0], ext[4] * spread[1]]
        for dx in (-1, 0, 1):
            moved = [near(s, dx, 0) for s in spread]
            for dy in (-1, 0, 1):
                if (dx, dy) == (0, 0):
                    continue
                share = cross_share * dx * dy
                for c in range(2):
                    val = moved[c] if share == 0 else moved[c] + share * moved[1 - c]
                    surface[c] = surface[c] + coef(dx, dy) * near(val, dy, 1)
        return surface

    def back(q, surface):
        traction = [ext[2] * s for s in surface]
        basal = [ext[4] * t for t in traction]
        for dx in (-1, 0, 1):
            part = [None, None]
            for dy in (-1, 0, 1):
                if (dx, dy) == (0, 0):
                    continue
                share = cross_share * dx * dy
                for c in range(2):
                    val = traction[c] if share == 0 else traction[c] + share * traction[1 - c]
                    val = near(coef(-dx, -dy) * val, dy, 1)
                    part[c] = val if part[c] is None else part[c] + val
            basal = [basal[c] + near(part[c], dx, 0) for c in range(2)]
        return ext[0] * basal[0] + ext[1] * basal[1] + regularize(q)

    def regularize(q):
        around = near(q, 1, 0) + near(q, -1, 0) + near(q, 1, 1) + near(q, -1, 1)
        return reg_gamma * (q + reg_smooth * (4.0 * q - around))

    def hessian(q):
        return back(q, forth(q))

    def mine(x):
        return x[rows:2 * rows, :cols]

    warm = ext[5]
    image = hessian(warm)
    r0 = ext[6] - image
    p0 = ext[3] * r0
    w0 = hessian(p0)
    y0 = ext[3] * w0
    surface = forth(y0)
    curve0 = mine(ext[2]) * (mine(surface[0]) * mine(surface[0]) + mine(surface[1]) * mine(surface[1])) + mine(y0 * regularize(y0))
    full_y0 = y0
    r0, p0, w0, y0 = mine(r0), mine(p0), mine(w0), mine(y0)

    def total(x):
        return jnp.sum(jnp.sum(x, axis=0, keepdims=True), axis=1, keepdims=True)

    one_lane = lax.broadcasted_iota(jnp.int32, (1, 128), 1)
    sums = jnp.zeros((1, 128), jnp.float32)
    for j, val in enumerate((r0 * p0, p0 * w0, w0 * y0, curve0)):
        sums = jnp.where(one_lane == j, total(val), sums)
    red[...] = sums

    def to_peer(j, index):
        peer = lax.rem(me + j, n)
        return pltpu.make_async_remote_copy(
            src_ref=red, dst_ref=slots.at[index],
            send_sem=r_send.at[j], recv_sem=r_recv.at[index],
            device_id=(peer // ny, lax.rem(peer, ny)), device_id_type=MESH,
        )

    def send(j, c):
        to_peer(j, me).start()
        return c

    def receive(j, c):
        to_peer(j, lax.rem(me + j, n)).wait_recv()
        return c

    def sent(j, c):
        to_peer(j, me).wait_send()
        return c

    pl.semaphore_wait(all_in, ny - 1)
    lax.fori_loop(1, n, send, 0, unroll=4)
    u0 = mine(back(full_y0, surface))
    each("wait_send", [name for name, _ in kinds])
    lax.fori_loop(1, n, receive, 0, unroll=4)
    slots[me] = sums
    everyone = jnp.sum(slots[...], axis=0)

    def pick(j):
        return jnp.sum(jnp.where(one_lane == j, everyone, 0.0), axis=1, keepdims=True)

    rz0, pw, wy, yu = pick(0), pick(1), pick(2), pick(3)
    a0 = rz0 / pw
    rz1 = a0 * a0 * wy - rz0
    beta = rz1 / rz0
    more = 1.0 + beta
    curve = more * (more * pw - 2.0 * a0 * wy) + a0 * a0 * yu
    a1 = rz1 / curve
    out_ref[0] = a0 * p0 + a1 * (more * p0 - a0 * y0)
    out_ref[1] = -mine(image) - a0 * w0 - a1 * (more * w0 - a0 * u0)
    lax.fori_loop(1, n, sent, 0)


def solution(mesh):
    nx, ny = mesh.shape["gx"], mesh.shape["gy"]
    n = nx * ny

    def on_device(gradient, warm_start, viscosity, friction_coef, slide_dir, obs_weight, ice_mask, grounded):
        levels, rows, cols = viscosity.shape
        vmem = pl.BlockSpec(memory_space=pltpu.VMEM)
        f32 = lambda *shape: pltpu.VMEM(shape, jnp.float32)
        flat = (gradient, warm_start, viscosity, friction_coef, slide_dir, obs_weight, ice_mask, grounded)
        change = pl.pallas_call(
            functools.partial(kernel, nx, ny),
            out_shape=jax.ShapeDtypeStruct((2, rows, cols), jnp.float32),
            in_specs=[pl.BlockSpec(memory_space=pl.ANY)] * 8,
            out_specs=vmem,
            scratch_shapes=[
                *(pltpu.VMEM(a.shape, a.dtype) for a in flat),
                f32(levels, rows, cols), f32(levels, rows, cols),
                f32(levels, rows, cols), f32(levels, rows, cols),
                f32(levels + 2, rows, cols), f32(levels + 2, rows, cols),
                f32(2, 2 * levels, cols), f32(2, 2 * levels, cols),
                f32(FIELDS, rows, cols), f32(2, FIELDS, rows, cols),
                f32(2, rows, 128), f32(6, rows, 128),
                f32(8, rows, cols), f32(2, 8, rows, cols),
                f32(2, rows, 128), f32(6, rows, 128),
                f32(FIELDS + 8, 3 * rows, cols + 128),
                f32(1, 128), f32(n, 1, 128),
                pltpu.SemaphoreType.DMA((8,)),
                pltpu.SemaphoreType.DMA((24,)), pltpu.SemaphoreType.DMA((24,)),
                pltpu.SemaphoreType.DMA((n,)), pltpu.SemaphoreType.DMA((n,)),
                pltpu.SemaphoreType.REGULAR,
            ],
            compiler_params=pltpu.CompilerParams(collective_id=0, has_side_effects=True),
        )(*flat)
        return warm_start + change[0], gradient + change[1]

    flat = P("gx", "gy")
    deep = P(None, "gx", "gy")
    return jax.shard_map(
        on_device,
        mesh=mesh,
        in_specs=(flat, flat, deep, flat, deep, flat, flat, flat),
        out_specs=(flat, flat),
        check_vma=False,
    )
```

```python
import functools

import jax
import jax.numpy as jnp
from jax import lax
from jax.experimental import pallas as pl
from jax.experimental.pallas import tpu as pltpu
from jax.sharding import PartitionSpec as P

vert_coupling = 128.0
sink_rate = 0.0625
bed_drag = 0.5
offset_weight = 0.0019
cross_share = 0.5
reg_gamma = 0.02
reg_smooth = 1.0
diag_scale = 0.003

MESH = pl.DeviceIdType.MESH
REACH = 6
DIRS = [(-1, 0), (1, 0), (0, -1), (0, 1), (-1, -1), (-1, 1), (1, -1), (1, 1)]
OPPOSITE = [1, 0, 3, 2, 7, 6, 5, 4]
FIELDS = 7


def roll(x, shift, axis):
    size = x.shape[axis]
    if isinstance(shift, int):
        shift = shift % size
        if shift == 0:
            return x
    return pltpu.roll(x, shift, axis)


def near(x, step, axis):
    return roll(x, -step, axis)


def kernel(
    nx, ny,
    grad_in, warm_in, visc_in, fric_in, slide_in, obs_in, ice_in, ground_in,
    out_ref,
    grad_ref, warm_ref, visc_ref, fric_ref, slide_ref, obs_ref, ice_ref, ground_ref,
    up, down, bot, gbot, top, gtop,
    t_row, row_send, row_recv, f_send, f_recv, p_send, p_recv, k_send, k_recv, kp_send, kp_recv,
    ext, red, slots,
    load_sem, s_send, s_recv, r_send, r_recv, all_in,
):
    levels, rows, cols = visc_ref.shape
    n = nx * ny
    ix, iy = lax.axis_index("gx"), lax.axis_index("gy")
    me = ix * ny + iy

    loads = [
        pltpu.make_async_copy(src, dst, load_sem.at[j])
        for j, (src, dst) in enumerate((
            (visc_in, visc_ref), (fric_in, fric_ref), (ground_in, ground_ref), (ice_in, ice_ref),
            (slide_in, slide_ref), (obs_in, obs_ref), (warm_in, warm_ref), (grad_in, grad_ref),
        ))
    ]

    def exists(d):
        dx, dy = DIRS[d]
        x, y = ix + dx, iy + dy
        return (x >= 0) & (x < nx) & (y >= 0) & (y < ny)

    barrier = pltpu.get_barrier_semaphore()

    def greet(x, y):
        pl.semaphore_signal(barrier, inc=1, device_id=(x, y), device_id_type=MESH)

    for load in loads:
        load.start()
    expected = nx - 1 + ny - 1
    for d in range(4, 8):
        expected = expected + exists(d).astype(jnp.int32)

        @pl.when(exists(d))
        def _():
            greet(ix + DIRS[d][0], iy + DIRS[d][1])
    for k in range(1, nx):
        greet(lax.rem(ix + k, nx), iy)
    for k in range(1, ny):
        greet(ix, lax.rem(iy + k, ny))

    def copy(src, dst, d, sem):
        dx, dy = DIRS[d]
        return pltpu.make_async_remote_copy(
            src_ref=src, dst_ref=dst,
            send_sem=s_send.at[sem + d], recv_sem=s_recv.at[sem + OPPOSITE[d]],
            device_id=(jnp.clip(ix + dx, 0, nx - 1), jnp.clip(iy + dy, 0, ny - 1)),
            device_id_type=MESH,
        )

    def message(d, what):
        o = OPPOSITE[d]
        side = 0 if DIRS[d][1] < 0 else 1
        return {
            "row": lambda: copy(row_send.at[d], row_recv.at[o], d, 0),
            "field": lambda: copy(f_send, f_recv.at[o], d, 8),
            "coef": lambda: copy(k_send, k_recv.at[o], d, 16),
            "pack": lambda: copy(p_send.at[side], p_recv.at[o - 2], d, 0),
            "coefpack": lambda: copy(kp_send.at[side], kp_recv.at[o - 2], d, 16),
        }[what]()

    beside_x, others = (0, 1), range(2, 8)
    kinds = (("row", beside_x), ("pack", others), ("field", beside_x), ("coefpack", others), ("coef", beside_x))

    def each(action, names):
        for name, towards in kinds:
            if name not in names:
                continue
            for d in towards:
                @pl.when(exists(d))
                def _():
                    if action == "wait_recv":
                        message(OPPOSITE[d], name).wait_recv()
                    elif action == "wait_send":
                        message(d, name).wait_send()
                    else:
                        message(d, name).start()

    def clear(ref):
        ref[...] = jnp.zeros(ref.shape, jnp.float32)

    for d in range(8):
        @pl.when(jnp.logical_not(exists(d)))
        def _():
            for ref in (row_recv, f_recv, k_recv) if d < 2 else (p_recv, kp_recv):
                clear(ref.at[d if d < 2 else d - 2])

    for load in loads:
        load.wait()

    ice = ice_ref[...].astype(jnp.float32)
    ground = ground_ref[...].astype(jnp.float32)
    fric = fric_ref[...]
    friction = ground * fric
    base = ice * ground * fric
    inverse = 1.0 / (reg_gamma * (1.0 + 4.0 * reg_smooth) + diag_scale * base * fric)
    lane = lax.broadcasted_iota(jnp.int32, (rows, 128), 1)

    def eliminate(i, carry):
        e, f = carry
        k = levels - 2 - i
        v_low, v_up = visc_ref[i], visc_ref[i + 1]
        link = (vert_coupling * 0.5) * (v_low + v_up)
        ratio = link / (link + e)
        up[i] = ratio
        e = sink_rate * v_up + e * ratio
        w_low, w_up = visc_ref[k], visc_ref[k + 1]
        link = (vert_coupling * 0.5) * (w_low + w_up)
        ratio = link / (link + f)
        down[k] = ratio
        f = sink_rate * w_low + f * ratio
        return e, f

    e = sink_rate * visc_ref[0] + bed_drag * friction
    f = sink_rate * visc_ref[levels - 1]
    e, f = lax.fori_loop(0, levels - 1, eliminate, (e, f), unroll=True)

    zero = jnp.zeros((rows, cols), jnp.float32)
    for ref in (top, gtop):
        ref[0] = zero
        ref[levels + 1] = zero

    def respond(z, carry):
        b, t, left, right, tleft, tright = carry
        g = visc_ref[z] * b
        bot[z] = b
        gbot[z] = g
        for j, val in ((0, b), (levels, g)):
            row_send[0, pl.ds(z + j, 1), :] = val[:1]
            row_send[1, pl.ds(z + j, 1), :] = val[rows - 1:]
            left = jnp.where(lane == z + j, roll(val[:, :128], z + j, 1), left)
            right = jnp.where(lane == z + j, roll(val[:, cols - 128:], z + j + 1, 1), right)
        k = levels - 1 - z
        top[k + 1] = t
        h = visc_ref[k] * t
        gtop[k + 1] = h
        for j, val in ((0, h), (levels, t)):
            t_row[0, pl.ds(k + j, 1), :] = val[:1]
            t_row[1, pl.ds(k + j, 1), :] = val[rows - 1:]
            tleft = jnp.where(lane == k + j, roll(val[:, :128], k + j, 1), tleft)
            tright = jnp.where(lane == k + j, roll(val[:, cols - 128:], k + j + 1, 1), tright)
        t = t * up[jnp.maximum(k - 1, 0)]
        b = b * down[jnp.minimum(z, levels - 2)]
        return b, t, left, right, tleft, tright

    blank = jnp.zeros((rows, 128), jnp.float32)
    _, _, left, right, tleft, tright = lax.fori_loop(
        0, levels, respond, (1.0 / (f + bed_drag * friction), 1.0 / e, blank, blank, blank, blank), unroll=4
    )

    own = [base * slide_ref[0], base * slide_ref[1], ice * obs_ref[...], inverse, bot[levels - 1], warm_ref[...], grad_ref[...]]

    def pack(fields, place, left, right):
        for val in fields:
            here = (lane >= place) & (lane < place + REACH)
            left = jnp.where(here, roll(val[:, :128], place, 1), left)
            right = jnp.where(here, roll(val[:, cols - 128:], place - (128 - REACH), 1), right)
            place += REACH
        return left, right

    left, right = pack(own, 2 * levels, left, right)
    for j, val in enumerate(own):
        f_send[j] = val
    p_send[0] = left
    p_send[1] = right

    pl.semaphore_wait(barrier, expected)
    each("start", ("row", "pack", "field"))
    for k in range(1, ny):
        pl.semaphore_signal(all_in, inc=1, device_id=(ix, lax.rem(iy + k, ny)), device_id_type=MESH)

    row_id = lax.broadcasted_iota(jnp.int32, (rows, cols), 0)
    col_id = lax.broadcasted_iota(jnp.int32, (rows, cols), 1)
    prow = lax.broadcasted_iota(jnp.int32, (rows, 128), 0)

    def beside(side):
        at = {dx: p_recv[DIRS.index((dx, side)) - 2] for dx in (-1, 0, 1)}
        return {
            -1: jnp.where(prow == 0, near(at[-1], -1, 0), near(at[0], -1, 0)),
            0: at[0],
            1: jnp.where(prow == rows - 1, near(at[1], 1, 0), near(at[0], 1, 0)),
        }

    def weigh(mid, out):
        return (
            (0.5 * offset_weight) * mid + (0.25 * offset_weight) * out,
            (0.25 * offset_weight) * mid + (0.5 * offset_weight / 3.0) * out,
        )

    def gather(z, acc):
        acc = list(acc)
        weights = [weigh(ref[z + 1], ref[z] + ref[z + 2]) for ref in (gtop, top)]
        for ref, weight in ((bot, weights[0]), (gbot, weights[1])):
            mid = ref[z]
            low = jnp.where(row_id == 0, 0.0, near(mid, -1, 0))
            high = jnp.where(row_id == rows - 1, 0.0, near(mid, 1, 0))
            for dx, val in ((-1, low), (0, mid), (1, high)):
                for dy in (-1, 0, 1):
                    if (dx, dy) != (0, 0):
                        d = DIRS.index((dx, dy))
                        moved = val if dy == 0 else near(val, dy, 1)
                        acc[d] = acc[d] + weight[1 if dx * dy != 0 else 0] * moved
        return tuple(acc)

    coefs = list(lax.fori_loop(0, levels, gather, (zero,) * 8, unroll=4))
    for d, (dx, dy) in enumerate(DIRS):
        if dy != 0:
            coefs[d] = jnp.where(col_id == (0 if dy < 0 else cols - 1), 0.0, coefs[d])

    layer = lax.broadcasted_iota(jnp.int32, (2 * levels, cols), 0)
    edge_col = lax.broadcasted_iota(jnp.int32, (2 * levels, cols), 1)

    def above_below(mid, index, axis):
        low = (index == 0) | (index == levels) | (index >= 2 * levels)
        high = (index == levels - 1) | (index >= 2 * levels - 1)
        return jnp.where(low, 0.0, near(mid, -1, axis)) + jnp.where(high, 0.0, near(mid, 1, axis))

    row_weights = [weigh(t_row[i], above_below(t_row[i], layer, 0)) for i in (0, 1)]
    col_weights = [weigh(t, above_below(t, lane, 1)) for t in (tleft, tright)]
    each("wait_recv", ("row", "pack"))
    for i, dx in enumerate((-1, 1)):
        halo = row_recv[i]
        for dy in (-1, 0, 1):
            d = DIRS.index((dx, dy))
            val = halo
            if dy != 0:
                val = jnp.where(edge_col == (0 if dy < 0 else cols - 1), 0.0, near(halo, dy, 1))
            part = jnp.sum(row_weights[i][1 if dy != 0 else 0] * val, axis=0, keepdims=True)
            coefs[d] = coefs[d] + jnp.where(row_id == (0 if dx < 0 else rows - 1), part, 0.0)
    for i, dy in enumerate((-1, 1)):
        at = beside(dy)
        for dx in (-1, 0, 1):
            d = DIRS.index((dx, dy))
            part = jnp.sum(col_weights[i][1 if dx != 0 else 0] * at[dx], axis=1, keepdims=True)
            coefs[d] = coefs[d] + jnp.where(col_id == (0 if dy < 0 else cols - 1), part, 0.0)
    for d in range(8):
        k_send[d] = coefs[d]
    kleft, kright = pack(coefs, 0, blank, blank)
    kp_send[0] = kleft
    kp_send[1] = kright
    each("start", ("coefpack", "coef"))

    def extend(j, mine, recv, packs_ref, index, place):
        for tile, dx in enumerate((-1, 0, 1)):
            here = mine if dx == 0 else recv[0 if dx < 0 else 1, index]
            from_right = packs_ref[DIRS.index((dx, 1)) - 2]
            from_left = packs_ref[DIRS.index((dx, -1)) - 2]
            halo = jnp.where(lane < REACH, roll(from_right, -place, 1), 0.0)
            halo = jnp.where(lane >= 128 - REACH, roll(from_left, 128 - REACH - place, 1), halo)
            ext[j, tile * rows:(tile + 1) * rows, :cols] = here
            ext[j, tile * rows:(tile + 1) * rows, cols:] = halo

    each("wait_recv", ("field",))
    for j in range(FIELDS):
        extend(j, f_send[j], f_recv, p_recv, j, 2 * levels + REACH * j)
    each("wait_recv", ("coefpack", "coef"))
    for d in range(8):
        extend(FIELDS + d, k_send[d], k_recv, kp_recv, d, REACH * d)

    def coef(dx, dy):
        return ext[FIELDS + DIRS.index((dx, dy))]

    def forth(q):
        spread = [ext[0] * q, ext[1] * q]
        surface = [ext[4] * spread[0], ext[4] * spread[1]]
        for dx in (-1, 0, 1):
            moved = [near(s, dx, 0) for s in spread]
            for dy in (-1, 0, 1):
                if (dx, dy) == (0, 0):
                    continue
                share = cross_share * dx * dy
                for c in range(2):
                    val = moved[c] if share == 0 else moved[c] + share * moved[1 - c]
                    surface[c] = surface[c] + coef(dx, dy) * near(val, dy, 1)
        return surface

    def back(q, surface):
        traction = [ext[2] * s for s in surface]
        basal = [ext[4] * t for t in traction]
        for dx in (-1, 0, 1):
            part = [None, None]
            for dy in (-1, 0, 1):
                if (dx, dy) == (0, 0):
                    continue
                share = cross_share * dx * dy
                for c in range(2):
                    val = traction[c] if share == 0 else traction[c] + share * traction[1 - c]
                    val = near(coef(-dx, -dy) * val, dy, 1)
                    part[c] = val if part[c] is None else part[c] + val
            basal = [basal[c] + near(part[c], dx, 0) for c in range(2)]
        return ext[0] * basal[0] + ext[1] * basal[1] + regularize(q)

    def regularize(q):
        around = near(q, 1, 0) + near(q, -1, 0) + near(q, 1, 1) + near(q, -1, 1)
        return reg_gamma * (q + reg_smooth * (4.0 * q - around))

    def hessian(q):
        return back(q, forth(q))

    def mine(x):
        return x[rows:2 * rows, :cols]

    warm = ext[5]
    image = hessian(warm)
    r0 = ext[6] - image
    p0 = ext[3] * r0
    w0 = hessian(p0)
    y0 = ext[3] * w0
    surface = forth(y0)
    curve0 = mine(ext[2]) * (mine(surface[0]) * mine(surface[0]) + mine(surface[1]) * mine(surface[1])) + mine(y0 * regularize(y0))
    full_y0 = y0
    r0, p0, w0, y0 = mine(r0), mine(p0), mine(w0), mine(y0)

    def total(x):
        return jnp.sum(jnp.sum(x, axis=0, keepdims=True), axis=1, keepdims=True)

    one_lane = lax.broadcasted_iota(jnp.int32, (1, 128), 1)
    sums = jnp.zeros((1, 128), jnp.float32)
    for j, val in enumerate((r0 * p0, p0 * w0, w0 * y0, curve0)):
        sums = jnp.where(one_lane == j, total(val), sums)
    red[...] = sums

    def to_peer(j, index):
        peer = lax.rem(me + j, n)
        return pltpu.make_async_remote_copy(
            src_ref=red, dst_ref=slots.at[index],
            send_sem=r_send.at[j], recv_sem=r_recv.at[index],
            device_id=(peer // ny, lax.rem(peer, ny)), device_id_type=MESH,
        )

    def send(j, c):
        to_peer(j, me).start()
        return c

    def receive(j, c):
        to_peer(j, lax.rem(me + j, n)).wait_recv()
        return c

    def sent(j, c):
        to_peer(j, me).wait_send()
        return c

    pl.semaphore_wait(all_in, ny - 1)
    lax.fori_loop(1, n, send, 0, unroll=4)
    u0 = mine(back(full_y0, surface))
    each("wait_send", [name for name, _ in kinds])
    lax.fori_loop(1, n, receive, 0, unroll=4)
    slots[me] = sums
    everyone = jnp.sum(slots[...], axis=0)

    def pick(j):
        return jnp.sum(jnp.where(one_lane == j, everyone, 0.0), axis=1, keepdims=True)

    rz0, pw, wy, yu = pick(0), pick(1), pick(2), pick(3)
    a0 = rz0 / pw
    rz1 = a0 * a0 * wy - rz0
    beta = rz1 / rz0
    more = 1.0 + beta
    curve = more * (more * pw - 2.0 * a0 * wy) + a0 * a0 * yu
    a1 = rz1 / curve
    out_ref[0] = a0 * p0 + a1 * (more * p0 - a0 * y0)
    out_ref[1] = -mine(image) - a0 * w0 - a1 * (more * w0 - a0 * u0)
    lax.fori_loop(1, n, sent, 0)


def solution(mesh):
    nx, ny = mesh.shape["gx"], mesh.shape["gy"]
    n = nx * ny

    def on_device(gradient, warm_start, viscosity, friction_coef, slide_dir, obs_weight, ice_mask, grounded):
        levels, rows, cols = viscosity.shape
        vmem = pl.BlockSpec(memory_space=pltpu.VMEM)
        f32 = lambda *shape: pltpu.VMEM(shape, jnp.float32)
        flat = (gradient, warm_start, viscosity, friction_coef, slide_dir, obs_weight, ice_mask, grounded)
        change = pl.pallas_call(
            functools.partial(kernel, nx, ny),
            out_shape=jax.ShapeDtypeStruct((2, rows, cols), jnp.float32),
            in_specs=[pl.BlockSpec(memory_space=pl.ANY)] * 8,
            out_specs=vmem,
            scratch_shapes=[
                *(pltpu.VMEM(a.shape, a.dtype) for a in flat),
                f32(levels, rows, cols), f32(levels, rows, cols),
                f32(levels, rows, cols), f32(levels, rows, cols),
                f32(levels + 2, rows, cols), f32(levels + 2, rows, cols),
                f32(2, 2 * levels, cols), f32(2, 2 * levels, cols), f32(2, 2 * levels, cols),
                f32(FIELDS, rows, cols), f32(2, FIELDS, rows, cols),
                f32(2, rows, 128), f32(6, rows, 128),
                f32(8, rows, cols), f32(2, 8, rows, cols),
                f32(2, rows, 128), f32(6, rows, 128),
                f32(FIELDS + 8, 3 * rows, cols + 128),
                f32(1, 128), f32(n, 1, 128),
                pltpu.SemaphoreType.DMA((8,)),
                pltpu.SemaphoreType.DMA((24,)), pltpu.SemaphoreType.DMA((24,)),
                pltpu.SemaphoreType.DMA((n,)), pltpu.SemaphoreType.DMA((n,)),
                pltpu.SemaphoreType.REGULAR,
            ],
            compiler_params=pltpu.CompilerParams(collective_id=0, has_side_effects=True),
        )(*flat)
        return warm_start + change[0], gradient + change[1]

    flat = P("gx", "gy")
    deep = P(None, "gx", "gy")
    return jax.shard_map(
        on_device,
        mesh=mesh,
        in_specs=(flat, flat, deep, flat, deep, flat, flat, flat),
        out_specs=(flat, flat),
        check_vma=False,
    )
```
